16 devices in a mesh: tp: 2 (over z), fsdp: 8 (over y, x, core).
Axes of the slice: x: 2, y: 2, z: 2, core: 2. Of those that a mesh axis runs over, the one named last changes fastest.
Arguments:
- x: bfloat16 [16, 512, 2048], P('fsdp')
- grad_y: bfloat16 [16, 512, 2048], P('fsdp')
- w_qkv: bfloat16 [2048, 3, 16, 128], P('fsdp', None, 'tp')
- w_out: bfloat16 [16, 128, 2048], P('tp', None, 'fsdp')
- w_ff: bfloat16 [2048, 2, 8192], P('fsdp', None, 'tp')
- w_down: bfloat16 [8192, 2048], P('tp', 'fsdp')
Outputs:
- output 1: bfloat16 [16, 512, 2048], P('fsdp')
- output 2: bfloat16 [16, 512, 2048], P('fsdp')
- output 3: float32 [2048, 3, 16, 128], P('fsdp', None, 'tp')
- output 4: float32 [16, 128, 2048], P('tp', None, 'fsdp')
- output 5: float32 [2048, 2, 8192], P('fsdp', None, 'tp')
- output 6: float32 [8192, 2048], P('tp', 'fsdp')
All inputs are finite; a program needn't handle non-finite values.
Results may differ from the reference program's by a relative error of at most 0.0163043.
Values are sent between devices in bfloat16 or wider.
A program may use at most 1 GiB of HBM per device.

```python
import jax
import jax.numpy as jnp
from jax import lax

BATCH = 16
SEQ = 512
D = 2048
HEADS = 16
HEAD = 128
FF = 8192
CLIP = 8.0
EPS = 1e-5
THETA = 10000.0


def setup_inputs(seed: int = 0) -> dict:
    rng_keys = jax.random.split(jax.random.key(seed), 6)
    x = jax.random.normal(rng_keys[0], (BATCH, SEQ, D), jnp.float32)
    grad_y = jax.random.normal(rng_keys[1], (BATCH, SEQ, D), jnp.float32)
    part_scale = jnp.array([1.0, 1.0, 5.0], jnp.float32)[None, :, None, None]
    w_qkv = jax.random.normal(rng_keys[2], (D, 3, HEADS, HEAD), jnp.float32) * (D ** -0.5) * part_scale
    w_out = jax.random.normal(rng_keys[3], (HEADS, HEAD, D), jnp.float32) * (2.0 * D ** -0.5)
    w_ff = jax.random.normal(rng_keys[4], (D, 2, FF), jnp.float32) * (D ** -0.5)
    w_down = jax.random.normal(rng_keys[5], (FF, D), jnp.float32) * (FF ** -0.5)
    return {'x': x.astype(jnp.bfloat16), 'grad_y': grad_y.astype(jnp.bfloat16), 'w_qkv': w_qkv.astype(jnp.bfloat16), 'w_out': w_out.astype(jnp.bfloat16), 'w_ff': w_ff.astype(jnp.bfloat16), 'w_down': w_down.astype(jnp.bfloat16)}


def layer_norm(values):
    mean_val = jnp.mean(values, axis=-1, keepdims=True)
    centered = values - mean_val
    variance = jnp.mean(centered * centered, axis=-1, keepdims=True)
    return centered * lax.rsqrt(variance + EPS)


def rope_tables():
    inv_freq = THETA ** (-jnp.arange(0, HEAD, 2, dtype=jnp.float32) / HEAD)
    angles = jnp.arange(SEQ, dtype=jnp.float32)[:, None] * inv_freq[None, :]
    return jnp.cos(angles)[:, None, :], jnp.sin(angles)[:, None, :]


def rotate(values, cos_tab, sin_tab):
    half_dim = HEAD // 2
    x_first = values[..., :half_dim]
    x_second = values[..., half_dim:]
    return jnp.concatenate([x_first * cos_tab - x_second * sin_tab, x_second * cos_tab + x_first * sin_tab], axis=-1)


def sequence_layer(x_seq, w_qkv, w_out, w_ff, w_down):
    cos_tab, sin_tab = rope_tables()
    normed1 = layer_norm(x_seq.astype(jnp.float32)).astype(jnp.bfloat16)
    qkv_raw = jnp.dot(normed1, w_qkv.astype(jnp.bfloat16).reshape(D, 3 * D), preferred_element_type=jnp.float32)
    qkv_cl = jnp.clip(qkv_raw, -CLIP, CLIP).reshape(SEQ, 3, HEADS, HEAD)
    q_rot = rotate(qkv_cl[:, 0], cos_tab, sin_tab).astype(jnp.bfloat16)
    k_rot = rotate(qkv_cl[:, 1], cos_tab, sin_tab).astype(jnp.bfloat16)
    v_val = qkv_cl[:, 2].astype(jnp.bfloat16)
    scores = jnp.einsum('qhe,khe->hqk', q_rot.astype(jnp.float32), k_rot.astype(jnp.float32)) * (HEAD ** -0.5)
    causal = jnp.arange(SEQ)[:, None] >= jnp.arange(SEQ)[None, :]
    scores = jnp.where(causal[None], scores, -1e30)
    prob_b16 = jax.nn.softmax(scores, axis=-1).astype(jnp.bfloat16)
    attn_o = jnp.einsum('hqk,khe->qhe', prob_b16.astype(jnp.float32), v_val.astype(jnp.float32)).astype(jnp.bfloat16)
    attn_proj = jnp.dot(attn_o.reshape(SEQ, D), w_out.astype(jnp.bfloat16).reshape(D, D), preferred_element_type=jnp.float32)
    hidden = (x_seq.astype(jnp.float32) + attn_proj).astype(jnp.bfloat16)
    normed2 = layer_norm(hidden.astype(jnp.float32)).astype(jnp.bfloat16)
    up_gate = jnp.dot(normed2, w_ff.astype(jnp.bfloat16).reshape(D, 2 * FF), preferred_element_type=jnp.float32).reshape(SEQ, 2, FF)
    mlp_act = (jax.nn.silu(up_gate[:, 1]) * up_gate[:, 0]).astype(jnp.bfloat16)
    mlp_proj = jnp.dot(mlp_act, w_down.astype(jnp.bfloat16), preferred_element_type=jnp.float32)
    return (hidden.astype(jnp.float32) + mlp_proj).astype(jnp.bfloat16)


def reference(x, grad_y, w_qkv, w_out, w_ff, w_down):
    def whole_layer(x_all, qkv_w, out_w, ff_w, down_w):
        layer_fn = jax.checkpoint(lambda x_seq: sequence_layer(x_seq, qkv_w, out_w, ff_w, down_w))
        return lax.map(layer_fn, x_all)

    y_out, pull_back = jax.vjp(whole_layer, x, w_qkv.astype(jnp.float32), w_out.astype(jnp.float32), w_ff.astype(jnp.float32), w_down.astype(jnp.float32))
    grad_x, grad_qkv, grad_out, grad_ff, grad_down = pull_back(grad_y)
    return y_out, grad_x, grad_qkv, grad_out, grad_ff, grad_down
```

```python
import functools

import jax
import jax.numpy as jnp
import numpy as np
from jax import lax
from jax.experimental import pallas as pl
from jax.experimental.pallas import tpu as pltpu
from jax.sharding import Mesh, PartitionSpec as P


F32 = jnp.float32
BF16 = jnp.bfloat16
SWAP = [(0, 1), (1, 0)]
EPS = 1e-5
CLIP = 8.0
SHARD = 256
VMEM_LIMIT = 60 * 1024 * 1024


def dot_nn(a, b):
    return lax.dot_general(a, b, (((1,), (0,)), ((), ())), preferred_element_type=F32)


def dot_nt(a, b):
    return lax.dot_general(a, b, (((1,), (1,)), ((), ())), preferred_element_type=F32)


def dot_tn(a, b):
    return lax.dot_general(a, b, (((0,), (0,)), ((), ())), preferred_element_type=F32)


def norm_stats(values):
    mean_val = jnp.mean(values, axis=-1, keepdims=True)
    centered = values - mean_val
    inv_std = lax.rsqrt(jnp.mean(centered * centered, axis=-1, keepdims=True) + EPS)
    return centered * inv_std, inv_std


def norm_backward(grad_norm, normed, inv_std):
    grad_mean = jnp.mean(grad_norm, axis=-1, keepdims=True)
    proj_mean = jnp.mean(grad_norm * normed, axis=-1, keepdims=True)
    return inv_std * (grad_norm - grad_mean - normed * proj_mean)


def call(kernel, grid, in_specs, out_specs, out_shape, ids, operands, flops, scratch=(), aliases=None):
    nbytes = sum(int(np.prod(o.shape)) * o.dtype.itemsize for o in operands)
    nbytes += sum(int(np.prod(o.shape)) * o.dtype.itemsize for o in jax.tree.leaves(out_shape))
    return pl.pallas_call(
        kernel,
        out_shape=out_shape,
        grid_spec=pltpu.PrefetchScalarGridSpec(
            num_scalar_prefetch=1, grid=grid, in_specs=in_specs, out_specs=out_specs, scratch_shapes=scratch
        ),
        input_output_aliases=aliases or {},
        compiler_params=pltpu.CompilerParams(
            dimension_semantics=('arbitrary',) * len(grid), vmem_limit_bytes=VMEM_LIMIT
        ),
        cost_estimate=pl.CostEstimate(flops=int(flops), bytes_accessed=int(nbytes), transcendentals=0),
    )(ids, *operands)


def sds(shape, dtype):
    return jax.ShapeDtypeStruct(shape, dtype)


def column_order(block, width):
    n = width // SHARD
    return [block[:, s * SHARD:(s + 1) * SHARD] for s in list(range(0, n, 2)) + list(range(1, n, 2))]


def ln1_kernel(ids, x_ref, gy_ref, n1_ref, xp_ref, gyp_ref):
    width = x_ref.shape[1]
    x = jnp.concatenate(column_order(x_ref, width), axis=1)
    xp_ref[...] = x
    gyp_ref[...] = jnp.concatenate(column_order(gy_ref, width), axis=1)
    normed, _ = norm_stats(x.astype(F32))
    n1_ref[...] = normed.astype(BF16)


def qkv_kernel(ids, n1_ref, w_ref, cos_ref, sin_ref, out_ref, keep_ref, *, rotated):
    raw = dot_nn(n1_ref[...], w_ref[...])
    keep_ref[...] = (jnp.abs(raw) < CLIP).astype(BF16)
    clipped = jnp.clip(raw, -CLIP, CLIP)
    seq, head = cos_ref.shape
    rows, cols = clipped.shape

    @pl.when(pl.program_id(0) < rotated)
    def _():
        for r in range(rows // seq):
            for c in range(cols // head):
                part = clipped[r * seq:(r + 1) * seq, c * head:(c + 1) * head]
                turned = part * cos_ref[...] + pltpu.roll(part, head // 2, 1) * sin_ref[...]
                out_ref[r * seq:(r + 1) * seq, c * head:(c + 1) * head] = turned.astype(BF16)

    @pl.when(pl.program_id(0) >= rotated)
    def _():
        out_ref[...] = clipped.astype(BF16)


def softmax_rows(q, k, first_row, scale):
    s = dot_nt(q, k) * scale
    row = first_row + lax.broadcasted_iota(jnp.int32, s.shape, 0)
    col = lax.broadcasted_iota(jnp.int32, s.shape, 1)
    s = jnp.where(row >= col, s, -1e30)
    e = jnp.exp(s - jnp.max(s, axis=-1, keepdims=True))
    return e / jnp.sum(e, axis=-1, keepdims=True)


def attn_kernel(ids, q_ref, k_ref, v_ref, o_ref, *, head, scale, rows):
    seq, cols = q_ref.shape
    for c in range(cols // head):
        cs = slice(c * head, (c + 1) * head)
        for r in range(seq // rows):
            rs = slice(r * rows, (r + 1) * rows)
            ks = slice(0, (r + 1) * rows)
            p = softmax_rows(q_ref[rs, cs], k_ref[ks, cs], r * rows, scale).astype(BF16)
            o_ref[rs, cs] = dot_nn(p, v_ref[ks, cs]).astype(BF16)


def attn_bwd_kernel(ids, q_ref, k_ref, v_ref, do_ref, keep_ref, cos_ref, sin_ref, out_ref, dk_acc, dv_acc, *, head, scale, rows):
    seq, cols = q_ref.shape
    for c in range(cols // head):
        cs = slice(c * head, (c + 1) * head)
        for r in reversed(range(seq // rows)):
            rs = slice(r * rows, (r + 1) * rows)
            ks = slice(0, (r + 1) * rows)
            q, k, v, do = q_ref[rs, cs], k_ref[ks, cs], v_ref[ks, cs], do_ref[rs, cs]
            p = softmax_rows(q, k, r * rows, scale)
            dp = dot_nt(do, v)
            ds = (p * (dp - jnp.sum(dp * p, axis=-1, keepdims=True)) * scale).astype(BF16)
            dv = dot_tn(p.astype(BF16), do)
            dk = dot_tn(ds, q)
            dq = dot_nn(ds, k)
            dq = dq * cos_ref[rs] - pltpu.roll(dq, head // 2, 1) * sin_ref[rs]
            out_ref[0, rs, cs] = jnp.where(keep_ref[0, rs, cs] > 0, dq, 0.0).astype(BF16)
            if r == seq // rows - 1:
                dk_acc[...] = dk
                dv_acc[...] = dv
            else:
                dk_acc[ks] += dk
                dv_acc[ks] += dv
        dk = dk_acc[...]
        dk = dk * cos_ref[...] - pltpu.roll(dk, head // 2, 1) * sin_ref[...]
        out_ref[1, :, cs] = jnp.where(keep_ref[1, :, cs] > 0, dk, 0.0).astype(BF16)
        out_ref[2, :, cs] = jnp.where(keep_ref[2, :, cs] > 0, dv_acc[...], 0.0).astype(BF16)


def nn_kernel(ids, *refs):
    *a_refs, w_ref, out_ref = refs
    depth = w_ref.shape[0] // len(a_refs)
    total = dot_nn(a_refs[0][...], w_ref[0:depth])
    for i, a_ref in enumerate(a_refs[1:], 1):
        total += dot_nn(a_ref[...], w_ref[i * depth:(i + 1) * depth])
    out_ref[...] = total


def combine1_kernel(ids, x_ref, part_ref, recv_ref, h_ref, n2_ref):
    h = (x_ref[...].astype(F32) + (part_ref[...] + recv_ref[...])).astype(BF16)
    h_ref[...] = h
    normed, _ = norm_stats(h.astype(F32))
    n2_ref[...] = normed.astype(BF16)


def ffn_kernel(ids, theirs_ref, mine_ref, wu_ref, wg_ref, u_ref, g_ref, act_ref, n2_ref):
    half = theirs_ref.shape[0]

    @pl.when(pl.program_id(0) == 0)
    def _():
        n2_ref[0:half] = theirs_ref[...]
        n2_ref[half:] = mine_ref[...]

    u = dot_nn(n2_ref[...], wu_ref[0])
    g = dot_nn(n2_ref[...], wg_ref[0])
    u_ref[...] = u
    g_ref[...] = g
    act_ref[...] = (g * jax.nn.sigmoid(g) * u).astype(BF16)


def dswiglu_kernel(ids, gy_ref, w_ref, u_ref, g_ref, out_ref):
    grad_act = dot_nt(gy_ref[...], w_ref[...])
    u, g = u_ref[...], g_ref[...]
    sig = jax.nn.sigmoid(g)
    out_ref[0] = (grad_act * (g * sig)).astype(BF16)
    out_ref[1] = (grad_act * u * sig * (1.0 + g * (1.0 - sig))).astype(BF16)


def grad_n2_kernel(ids, lo_ref, hi_ref, w_ref, out_ref):
    depth = lo_ref.shape[2]
    total = dot_nt(lo_ref[0], w_ref[0, :, 0:depth])
    total += dot_nt(hi_ref[0], w_ref[0, :, depth:])
    total += dot_nt(lo_ref[1], w_ref[1, :, 0:depth])
    total += dot_nt(hi_ref[1], w_ref[1, :, depth:])
    out_ref[...] = total


def combine2_kernel(ids, gy_ref, h_ref, part_ref, recv_ref, gh_ref, ghb_ref):
    normed, inv_std = norm_stats(h_ref[...].astype(F32))
    gh = gy_ref[...].astype(F32) + norm_backward(part_ref[...] + recv_ref[...], normed, inv_std)
    gh_ref[...] = gh
    ghb_ref[...] = gh.astype(BF16)


def grad_o_kernel(ids, theirs_ref, mine_ref, w_ref, out_ref, gh_ref):
    half = theirs_ref.shape[0]

    @pl.when(pl.program_id(0) == 0)
    def _():
        gh_ref[0:half] = theirs_ref[...]
        gh_ref[half:] = mine_ref[...]

    out_ref[...] = dot_nt(gh_ref[...], w_ref[...]).astype(BF16)


def grad_n1_kernel(ids, d_ref, w_ref, out_ref):
    depth = d_ref.shape[2]
    total = dot_nt(d_ref[0], w_ref[:, 0:depth])
    total += dot_nt(d_ref[1], w_ref[:, depth:2 * depth])
    total += dot_nt(d_ref[2], w_ref[:, 2 * depth:])
    out_ref[...] = total


def wgrad_rows_kernel(ids, a_ref, a2_ref, b_ref, b2_ref, *rest):
    *_, out_ref, at_ref = rest
    tokens = a_ref.shape[0]

    @pl.when((pl.program_id(0) == 0) & (pl.program_id(1) == 0))
    def _():
        at_ref[:, 0:tokens] = a_ref[...].T
        at_ref[:, tokens:] = a2_ref[...].T

    total = dot_nn(at_ref[:, 0:tokens], b_ref[0]) + dot_nn(at_ref[:, tokens:], b2_ref[0])
    out_ref[...] = total.reshape(out_ref.shape)


def wgrad_cols_kernel(ids, a_ref, a2_ref, b_ref, b2_ref, *rest):
    out_ref = rest[-1]
    total = dot_tn(a_ref[...], b_ref[...]) + dot_tn(a2_ref[...], b2_ref[...])
    for i in range(out_ref.shape[0]):
        out_ref[i] = total[:, i * SHARD:(i + 1) * SHARD]


def natural_order(values):
    n = values.shape[1] // SHARD
    blocks = [values[:, s * SHARD:(s + 1) * SHARD] for s in range(n)]
    return jnp.concatenate([blocks[(b % 2) * (n // 2) + b // 2] for b in range(n)], axis=1)


def y_kernel(ids, h_ref, part_ref, recv_ref, y_ref):
    y = (h_ref[...].astype(F32) + (part_ref[...] + recv_ref[...])).astype(BF16)
    y_ref[...] = natural_order(y)


def gx_kernel(ids, gh_ref, x_ref, part_ref, recv_ref, gx_ref):
    normed, inv_std = norm_stats(x_ref[...].astype(F32))
    gx = gh_ref[...] + norm_backward(part_ref[...] + recv_ref[...], normed, inv_std)
    gx_ref[...] = natural_order(gx.astype(BF16))


def other_z(value):
    return lax.ppermute(value, 'z', SWAP)


def other_core(value):
    return lax.ppermute(value, 'c', SWAP)


def after(value, *others):
    return lax.optimization_barrier((value,) + others)[0]


def gather(weight, axis):
    return lax.all_gather(weight, ('c', 'y', 'x'), axis=axis, tiled=True)


def scatter(grad, axis):
    return lax.psum_scatter(grad, ('y', 'x'), scatter_dimension=axis, tiled=True)


def layer(x, grad_y, w_qkv, w_out, w_ff, w_down):
    batch, seq, width = x.shape
    heads, head = w_qkv.shape[2:]
    inner = heads * head
    units = w_ff.shape[2]
    tokens = batch * seq
    half = tokens // 2
    chips = width // (2 * SHARD)
    z = lax.axis_index('z')
    core = lax.axis_index('c')
    ids = jnp.stack([z, core]).astype(jnp.int32)
    scale = head ** -0.5

    inv_freq = 10000.0 ** (-jnp.arange(0, head, 2, dtype=F32) / head)
    angles = jnp.arange(seq, dtype=F32)[:, None] * inv_freq[None, :]
    cos_tab = jnp.concatenate([jnp.cos(angles), jnp.cos(angles)], axis=1)
    sin_tab = jnp.concatenate([-jnp.sin(angles), jnp.sin(angles)], axis=1)

    qkv_full = gather(w_qkv.reshape(w_qkv.shape[0], 3 * inner), 0)
    out_full = gather(w_out.reshape(inner, w_out.shape[2]), 1)
    ff_full = gather(jnp.transpose(w_ff, (1, 0, 2)), 1)
    down_full = gather(w_down, 1)

    br = 128
    per_half = half // br
    src = lambda i, s: (((i // per_half + s[0] + 1) % 2) * per_half + i % per_half, 0)
    row = lambda i, s: (i, 0)
    n1, xp, gyp = call(
        ln1_kernel, (tokens // br,),
        [pl.BlockSpec((br, width), src)] * 2, [pl.BlockSpec((br, width), row)] * 3,
        [sds((tokens, width), BF16)] * 3, ids,
        [x.reshape(tokens, width), grad_y.reshape(tokens, width)], 20 * tokens * width)

    bn = 512
    fixed = lambda *_: (0, 0)
    n_qkv = 3 * inner // bn
    qkv, keep = call(
        functools.partial(qkv_kernel, rotated=2 * inner // bn), (n_qkv,),
        [pl.BlockSpec((tokens, width), fixed), pl.BlockSpec((width, bn), lambda j, s: (0, j)),
         pl.BlockSpec((seq, head), fixed), pl.BlockSpec((seq, head), fixed)],
        [pl.BlockSpec((tokens, bn), lambda j, s: (0, j)), pl.BlockSpec((None, tokens, bn), lambda j, s: (j // (n_qkv // 3), 0, j % (n_qkv // 3)))],
        [sds((tokens, 3 * inner), BF16), sds((3, tokens, inner), BF16)], ids,
        [n1, qkv_full, cos_tab, sin_tab], 2 * tokens * width * 3 * inner)

    bh = 256
    n_h = inner // bh
    qkv_spec = [pl.BlockSpec((seq, bh), lambda b, h, s, p=p: (b, p * n_h + h)) for p in range(3)]
    attn_o = call(
        functools.partial(attn_kernel, head=head, scale=scale, rows=256), (batch, n_h),
        qkv_spec, pl.BlockSpec((seq, bh), lambda b, h, s: (b, h)), sds((tokens, inner), BF16), ids,
        [qkv, qkv, qkv], 4 * tokens * seq * inner)

    def nn(lhs, w, r):
        depth = lhs[0].shape[1]
        return call(
            nn_kernel, (width // bn,),
            [pl.BlockSpec((half, depth), lambda j, s: (r, 0))] * len(lhs) + [pl.BlockSpec((depth * len(lhs), bn), lambda j, s: (0, j))],
            pl.BlockSpec((half, bn), lambda j, s: (0, j)), sds((half, width), F32), ids,
            [*lhs, w], 2 * half * depth * len(lhs) * width)

    part_theirs = nn([attn_o], out_full, 0)
    part_mine = nn([after(attn_o, part_theirs)], out_full, 1)
    mine_rows = lambda i, s: (per_half + i, 0)
    block = pl.BlockSpec((br, width), row)
    hidden, n2_mine = call(
        combine1_kernel, (per_half,), [pl.BlockSpec((br, width), mine_rows), block, block], [block, block],
        [sds((half, width), BF16)] * 2, ids, [xp, part_mine, other_z(part_theirs)], 20 * half * width)
    n2_theirs = other_z(n2_mine)

    bf = 256
    hu = units // 2

    def ffn(k, dep):
        nb = hu // bf
        up, gate, act, n2 = call(
            ffn_kernel, (nb,),
            [pl.BlockSpec((half, width), fixed)] * 2
            + [pl.BlockSpec((1, width, bf), lambda j, s, c=c: (c, 0, k * nb + j)) for c in range(2)],
            [pl.BlockSpec((tokens, bf), lambda j, s: (0, j))] * 3 + [pl.BlockSpec((tokens, width), fixed)],
            [sds((tokens, hu), F32)] * 2 + [sds((tokens, hu), BF16), sds((tokens, width), BF16)], ids,
            [after(n2_theirs, *dep), n2_mine, ff_full, ff_full], 4 * tokens * width * hu)
        return up, gate, act, n2

    up0, gate0, act0, n2 = ffn(0, ())
    up1, gate1, act1, _ = ffn(1, (act0,))
    act_sib = (other_core(act0), other_core(act1))
    gyp_sib = other_core(gyp)
    n2_sib = other_core(n2)
    n1_sib = other_core(n1)
    o_sib = other_core(attn_o)

    ba = 512
    mine_half = lambda *a: (0, a[-1][1])

    def wgrad_cols(a, a2, b, b2, total_rows, first, buf, dep):
        n = a.shape[1] // ba
        extra = [] if buf is None else [buf]
        return call(
            wgrad_cols_kernel, (n,),
            [pl.BlockSpec((tokens, ba), lambda j, s: (0, j))] * 2 + [pl.BlockSpec((tokens, width // 2), mine_half)] * 2
            + [pl.BlockSpec(memory_space=pl.ANY)] * len(extra),
            pl.BlockSpec((chips, ba, SHARD), lambda j, s: (0, first + j, 0)), sds((chips, total_rows, SHARD), F32), ids,
            [after(a, *dep), a2, b, b2, *extra], 4 * tokens * a.shape[1] * width // 2, aliases={5: 0} if extra else None)

    gd = wgrad_cols(act0, act_sib[0], gyp, gyp_sib, units, 0, None, (act1,))
    gd = wgrad_cols(act1, act_sib[1], gyp, gyp_sib, units, hu // ba, gd, ())
    grad_down = scatter(gd.reshape(chips * units, SHARD), 0)

    def dswiglu(k, up, gate, dep):
        nb = hu // bf
        return call(
            dswiglu_kernel, (nb,),
            [pl.BlockSpec((tokens, width), fixed), pl.BlockSpec((bf, width), lambda j, s: (k * nb + j, 0))]
            + [pl.BlockSpec((tokens, bf), lambda j, s: (0, j))] * 2,
            pl.BlockSpec((2, tokens, bf), lambda j, s: (0, 0, j)), sds((2, tokens, hu), BF16), ids,
            [after(gyp, *dep), down_full, up, gate], 2 * tokens * width * hu)

    d0 = dswiglu(0, up0, gate0, (gd,))
    d1 = dswiglu(1, up1, gate1, (d0,))
    d0_sib = other_core(d0)
    d1_sib = other_core(d1)

    def grad_n2(r, dep):
        bd = 256
        return call(
            grad_n2_kernel, (width // bd,),
            [pl.BlockSpec((2, half, hu), lambda j, s: (0, r, 0))] * 2 + [pl.BlockSpec((2, bd, units), lambda j, s: (0, j, 0))],
            pl.BlockSpec((half, bd), lambda j, s: (0, j)), sds((half, width), F32), ids,
            [after(d0, *dep), d1, ff_full], 4 * half * width * units)

    gn2_theirs = grad_n2(0, ())
    gn2_mine = grad_n2(1, (gn2_theirs,))

    def wgrad_ff(k, b, b2, buf, dep):
        n = hu // bn
        extra = [] if buf is None else [buf]
        return call(
            wgrad_rows_kernel, (2, n),
            [pl.BlockSpec((tokens, width // 2), mine_half)] * 2 + [pl.BlockSpec((1, tokens, bn), lambda c, j, s: (c, 0, j))] * 2
            + [pl.BlockSpec(memory_space=pl.ANY)] * len(extra),
            pl.BlockSpec((1, width // 2, bn), lambda c, j, s: (c, 0, k * n + j)), sds((2, width // 2, units), F32), ids,
            [after(n2, *dep), n2_sib, b, b2, *extra], 8 * tokens * width // 2 * hu,
            scratch=[pltpu.VMEM((width // 2, 2 * tokens), BF16)], aliases={5: 0} if extra else None)

    gff = wgrad_ff(0, d0, d0_sib, None, (gn2_mine,))
    gff = wgrad_ff(1, d1, d1_sib, gff, ())
    grad_ff = jnp.transpose(scatter(gff, 1), (1, 0, 2))

    gh, gh_mine = call(
        combine2_kernel, (per_half,),
        [pl.BlockSpec((br, width), mine_rows), block, block, block], [block, block],
        [sds((half, width), F32), sds((half, width), BF16)], ids,
        [after(gyp, gff), hidden, gn2_mine, other_z(gn2_theirs)], 20 * half * width)

    y_theirs = nn([after(act0, gh_mine), act1], down_full, 0)
    y_mine = nn([after(act0, y_theirs), act1], down_full, 1)

    grad_o, ghb = call(
        grad_o_kernel, (inner // bn,),
        [pl.BlockSpec((half, width), fixed)] * 2 + [pl.BlockSpec((bn, width), lambda j, s: (j, 0))],
        [pl.BlockSpec((tokens, bn), lambda j, s: (0, j)), pl.BlockSpec((tokens, width), fixed)],
        [sds((tokens, inner), BF16), sds((tokens, width), BF16)], ids,
        [other_z(gh_mine), after(gh_mine, y_mine), out_full], 2 * tokens * width * inner)
    gh_sib = other_core(ghb)
    dqkv = call(
        functools.partial(attn_bwd_kernel, head=head, scale=scale, rows=256), (batch, n_h),
        qkv_spec + [pl.BlockSpec((seq, bh), lambda b, h, s: (b, h)), pl.BlockSpec((3, seq, bh), lambda b, h, s: (0, b, h)),
                    pl.BlockSpec((seq, head), fixed), pl.BlockSpec((seq, head), fixed)],
        pl.BlockSpec((3, seq, bh), lambda b, h, s: (0, b, h)), sds((3, tokens, inner), BF16), ids,
        [qkv, qkv, qkv, grad_o, keep, cos_tab, sin_tab], 10 * tokens * seq * inner,
        scratch=[pltpu.VMEM((seq, head), F32)] * 2)
    dqkv_sib = other_core(dqkv)

    def grad_n1(r, dep):
        return call(
            grad_n1_kernel, (width // bn,),
            [pl.BlockSpec((3, half, inner), lambda j, s: (0, r, 0)), pl.BlockSpec((bn, 3 * inner), lambda j, s: (j, 0))],
            pl.BlockSpec((half, bn), lambda j, s: (0, j)), sds((half, width), F32), ids,
            [after(dqkv, *dep), qkv_full], 2 * half * width * 3 * inner)

    gn1_theirs = grad_n1(0, ())
    gn1_mine = grad_n1(1, (gn1_theirs,))
    go = wgrad_cols(attn_o, o_sib, ghb, gh_sib, inner, 0, None, (gn1_mine,))
    grad_out = scatter(go.reshape(chips * inner, SHARD), 0).reshape(heads, head, SHARD)
    gq = call(
        wgrad_rows_kernel, (3, inner // bn),
        [pl.BlockSpec((tokens, width // 2), mine_half)] * 2 + [pl.BlockSpec((1, tokens, bn), lambda c, j, s: (c, 0, j))] * 2,
        pl.BlockSpec((width // 2, bn), lambda c, j, s: (0, c * (inner // bn) + j)), sds((width // 2, 3 * inner), F32), ids,
        [after(n1, go), n1_sib, dqkv, dqkv_sib], 4 * tokens * width // 2 * 3 * inner,
        scratch=[pltpu.VMEM((width // 2, 2 * tokens), BF16)])
    grad_qkv = scatter(gq, 0).reshape(SHARD, 3, heads, head)

    def in_order(theirs, mine):
        both = jnp.where(z == 0, jnp.concatenate([mine, theirs], 0), jnp.concatenate([theirs, mine], 0))
        return both.reshape(batch, seq, width)

    y_own = call(
        y_kernel, (per_half,), [block] * 3, block, sds((half, width), BF16), ids,
        [after(hidden, gq), y_mine, other_z(y_theirs)], 4 * half * width)
    y_out = in_order(other_z(y_own), y_own)
    gx_own = call(
        gx_kernel, (per_half,), [block, pl.BlockSpec((br, width), mine_rows), block, block], block,
        sds((half, width), BF16), ids, [after(gh, y_own), xp, gn1_mine, other_z(gn1_theirs)], 20 * half * width)
    grad_x = in_order(other_z(gx_own), gx_own)
    return y_out, grad_x, grad_qkv, grad_out, grad_ff, grad_down


def solution(mesh):
    fine = Mesh(np.asarray(mesh.devices).reshape(2, 2, 2, 2), ('z', 'y', 'x', 'c'))
    fsdp = ('y', 'x', 'c')
    act_spec = P(fsdp, None, None)
    weight_specs = (P(fsdp, None, 'z', None), P('z', None, fsdp), P(fsdp, None, 'z'), P('z', fsdp))
    return jax.shard_map(layer, mesh=fine, in_specs=(act_spec, act_spec) + weight_specs, out_specs=(act_spec, act_spec) + weight_specs, check_vma=False)
```

```python
import functools

import jax
import jax.numpy as jnp
import numpy as np
from jax import lax
from jax.experimental import pallas as pl
from jax.experimental.pallas import tpu as pltpu
from jax.sharding import Mesh, PartitionSpec as P


F32 = jnp.float32
BF16 = jnp.bfloat16
SWAP = [(0, 1), (1, 0)]
EPS = 1e-5
CLIP = 8.0
SHARD = 256
ROLES = 14
OWN_ROLES = (0, 4, 1, 3, 6, 7)


VMEM_LIMIT = 60 * 1024 * 1024


def dot_nn(a, b):
    return lax.dot_general(a, b, (((1,), (0,)), ((), ())), preferred_element_type=F32)


def dot_nt(a, b):
    return lax.dot_general(a, b, (((1,), (1,)), ((), ())), preferred_element_type=F32)


def dot_tn(a, b):
    return lax.dot_general(a, b, (((0,), (0,)), ((), ())), preferred_element_type=F32)


def norm_stats(values):
    mean_val = jnp.mean(values, axis=-1, keepdims=True)
    centered = values - mean_val
    inv_std = lax.rsqrt(jnp.mean(centered * centered, axis=-1, keepdims=True) + EPS)
    return centered * inv_std, inv_std


def norm_backward(grad_norm, normed, inv_std):
    grad_mean = jnp.mean(grad_norm, axis=-1, keepdims=True)
    proj_mean = jnp.mean(grad_norm * normed, axis=-1, keepdims=True)
    return inv_std * (grad_norm - grad_mean - normed * proj_mean)


def call(kernel, grid, in_specs, out_specs, out_shape, ids, operands, flops, scratch=(), aliases=None, collective=None):
    nbytes = sum(int(np.prod(o.shape)) * o.dtype.itemsize for o in operands)
    nbytes += sum(int(np.prod(o.shape)) * o.dtype.itemsize for o in jax.tree.leaves(out_shape))
    return pl.pallas_call(
        kernel,
        out_shape=out_shape,
        grid_spec=pltpu.PrefetchScalarGridSpec(
            num_scalar_prefetch=0 if ids is None else 1, grid=grid, in_specs=in_specs, out_specs=out_specs, scratch_shapes=scratch
        ),
        input_output_aliases=aliases or {},
        compiler_params=pltpu.CompilerParams(
            dimension_semantics=('arbitrary',) * len(grid), vmem_limit_bytes=VMEM_LIMIT,
            collective_id=collective, has_side_effects=collective is not None,
        ),
        cost_estimate=pl.CostEstimate(flops=int(flops), bytes_accessed=int(nbytes), transcendentals=0),
    )(*([] if ids is None else [ids]), *operands)


def sds(shape, dtype):
    return jax.ShapeDtypeStruct(shape, dtype)


def column_order(block, width):
    n = width // SHARD
    return [block[:, s * SHARD:(s + 1) * SHARD] for s in list(range(0, n, 2)) + list(range(1, n, 2))]


class PlaneGather:
    def __init__(self, own, place, send_sem, recv_sem):
        y, x, core = lax.axis_index('y'), lax.axis_index('x'), lax.axis_index('c')
        self.targets = ({'x': 1 - x}, {'y': 1 - y}, {'c': 1 - core})
        self.own, self.send_sem, self.recv_sem = own, send_sem, recv_sem
        self.place = lambda flip_y, flip_x, h: place(core * 4 + (1 - y if flip_y else y) * 2 + (1 - x if flip_x else x), h)

    def copy(self, role):
        to_x, to_y, to_core = self.targets
        if role < 2:
            src, dst, target = self.own(role), self.place(0, 0, role), to_x
        elif role == 2:
            src, dst, target = self.place(1, 0, 1), self.place(1, 0, 1), to_x
        elif role < 5:
            src, dst, target = self.own(role - 3), self.place(0, 0, role - 3), to_y
        elif role == 5:
            src, dst, target = self.place(0, 1, 0), self.place(0, 1, 0), to_y
        elif role < 8:
            src, dst, target = self.own(role - 6), self.place(0, 0, role - 6), to_core
        else:
            flip_y, flip_x = ((0, 1), (1, 0), (1, 1))[(role - 8) // 2]
            src, dst, target = self.place(flip_y, flip_x, role % 2), self.place(flip_y, flip_x, role % 2), to_core
        return pltpu.make_async_remote_copy(src, dst, self.send_sem.at[role], self.recv_sem.at[role], device_id=target,
                                            device_id_type=pl.DeviceIdType.MESH)

    def meet(self):
        barrier = pltpu.get_barrier_semaphore()
        for target in self.targets:
            pl.semaphore_signal(barrier, inc=1, device_id=target, device_id_type=pl.DeviceIdType.MESH)
        pl.semaphore_wait(barrier, 3)

    def start(self):
        for role in OWN_ROLES:
            self.copy(role).start()

    def pass_on(self, pairs):
        for arrived, onward in pairs:
            self.copy(arrived).wait_recv()
            for role in onward:
                self.copy(role).start()

    def first(self):
        self.pass_on(((0, (5, 8)), (4, (2, 11))))

    def rest(self):
        self.pass_on(((1, (9,)), (3, (10,)), (5, (12,)), (2, (13,))))

    def finish(self):
        for role in range(6, ROLES):
            self.copy(role).wait_recv()
        for role in range(ROLES):
            self.copy(role).wait_send()


def q_gather(own_ref, full_ref, send_sem, recv_sem):
    n = own_ref.shape[0] // 2
    place = lambda shard, h: full_ref.at[pl.ds(pl.multiple_of((shard * 2 + h) * n, n), n)]
    return PlaneGather(lambda h: own_ref.at[pl.ds(h * n, n)], place, send_sem, recv_sem)


def o_gather(own_ref, full_ref, send_sem, recv_sem):
    n, cols = own_ref.shape[0] // 2, own_ref.shape[1]
    place = lambda shard, h: full_ref.at[shard // 4, pl.ds(h * n, n), pl.ds(pl.multiple_of(shard % 4 * cols, cols), cols)]
    return PlaneGather(lambda h: own_ref.at[pl.ds(h * n, n)], place, send_sem, recv_sem)


def own_shard():
    return lax.axis_index('c') * 4 + lax.axis_index('y') * 2 + lax.axis_index('x')


def head_kernel(x_ref, gy_ref, wf_ref, wq_ref, wo_ref, n1_ref, xp_ref, gyp_ref, ff_ref, q_full, o_full, wq_v, wo_v, local_sem, send_sem, recv_sem):
    step = pl.program_id(0)
    q_plan = q_gather(wq_ref, q_full, send_sem.at[0], recv_sem.at[0])
    o_plan = o_gather(wo_ref, o_full, send_sem.at[1], recv_sem.at[1])
    rows, cols = wq_ref.shape[0], wo_ref.shape[1]
    shard = own_shard()
    loads = [pltpu.make_async_copy(wq_ref, wq_v, local_sem.at[0]), pltpu.make_async_copy(wo_ref, wo_v, local_sem.at[1])]
    stores = [
        pltpu.make_async_copy(wq_v, q_full.at[pl.ds(pl.multiple_of(shard * rows, rows), rows)], local_sem.at[2]),
        pltpu.make_async_copy(wo_v, o_full.at[shard // 4, :, pl.ds(pl.multiple_of(shard % 4 * cols, cols), cols)], local_sem.at[3]),
    ]

    @pl.when(step == 0)
    def _():
        q_plan.meet()
        q_plan.start()
        for load in loads:
            load.start()

    values = jnp.concatenate(column_order(x_ref, x_ref.shape[1]), axis=1)
    xp_ref[...] = values
    gyp_ref[...] = jnp.concatenate(column_order(gy_ref, gy_ref.shape[1]), axis=1)
    normed, _ = norm_stats(values.astype(F32))
    n1_ref[...] = normed.astype(BF16)
    ff_ref[0] = wf_ref[:, 0, :]
    ff_ref[1] = wf_ref[:, 1, :]

    @pl.when(step == pl.num_programs(0) - 1)
    def _():
        for load, store in zip(loads, stores):
            load.wait()
            store.start()
        q_plan.first()
        o_plan.start()
        q_plan.rest()
        o_plan.first()
        o_plan.rest()
        q_plan.finish()
        o_plan.finish()
        for store in stores:
            store.wait()


def qkv_kernel(ids, n1_ref, w_ref, cos_ref, sin_ref, *rest, rotated):
    out_ref, keep_ref = rest[-2:]
    raw = dot_nn(n1_ref[...], w_ref[...])
    keep_ref[...] = (jnp.abs(raw) < CLIP).astype(BF16)
    clipped = jnp.clip(raw, -CLIP, CLIP)
    seq, head = cos_ref.shape
    rows, cols = clipped.shape

    @pl.when(pl.program_id(0) < rotated)
    def _():
        for r in range(rows // seq):
            for c in range(cols // head):
                part = clipped[r * seq:(r + 1) * seq, c * head:(c + 1) * head]
                turned = part * cos_ref[...] + pltpu.roll(part, head // 2, 1) * sin_ref[...]
                out_ref[r * seq:(r + 1) * seq, c * head:(c + 1) * head] = turned.astype(BF16)

    @pl.when(pl.program_id(0) >= rotated)
    def _():
        out_ref[...] = clipped.astype(BF16)


def softmax_rows(q, k, first_row, scale):
    s = dot_nt(q, k) * scale
    row = first_row + lax.broadcasted_iota(jnp.int32, s.shape, 0)
    col = lax.broadcasted_iota(jnp.int32, s.shape, 1)
    s = jnp.where(row >= col, s, -1e30)
    e = jnp.exp(s - jnp.max(s, axis=-1, keepdims=True))
    return e / jnp.sum(e, axis=-1, keepdims=True)


def attn_kernel(ids, q_ref, k_ref, v_ref, *rest, head, scale, rows, send):
    o_ref = rest[-1]
    seq, cols = q_ref.shape
    for c in range(cols // head):
        cs = slice(c * head, (c + 1) * head)
        for r in range(seq // rows):
            rs = slice(r * rows, (r + 1) * rows)
            ks = slice(0, (r + 1) * rows)
            p = softmax_rows(q_ref[rs, cs], k_ref[ks, cs], r * rows, scale).astype(BF16)
            o = dot_nn(p, v_ref[ks, cs]).astype(BF16)
            o_ref[rs, cs] = o
            if send:
                rest[-2][rs, cs] = o


def attn_bwd_kernel(ids, q_ref, k_ref, v_ref, do_ref, keep_ref, cos_ref, sin_ref, out_ref, dk_acc, dv_acc, *, head, scale, rows):
    seq, cols = q_ref.shape
    for c in range(cols // head):
        cs = slice(c * head, (c + 1) * head)
        for r in reversed(range(seq // rows)):
            rs = slice(r * rows, (r + 1) * rows)
            ks = slice(0, (r + 1) * rows)
            q, k, v, do = q_ref[rs, cs], k_ref[ks, cs], v_ref[ks, cs], do_ref[rs, cs]
            p = softmax_rows(q, k, r * rows, scale)
            dp = dot_nt(do, v)
            ds = (p * (dp - jnp.sum(dp * p, axis=-1, keepdims=True)) * scale).astype(BF16)
            dv = dot_tn(p.astype(BF16), do)
            dk = dot_tn(ds, q)
            dq = dot_nn(ds, k)
            dq = dq * cos_ref[rs] - pltpu.roll(dq, head // 2, 1) * sin_ref[rs]
            out_ref[0, rs, cs] = jnp.where(keep_ref[0, rs, cs] > 0, dq, 0.0).astype(BF16)
            if r == seq // rows - 1:
                dk_acc[...] = dk
                dv_acc[...] = dv
            else:
                dk_acc[ks] += dk
                dv_acc[ks] += dv
        dk = dk_acc[...]
        dk = dk * cos_ref[...] - pltpu.roll(dk, head // 2, 1) * sin_ref[...]
        out_ref[1, :, cs] = jnp.where(keep_ref[1, :, cs] > 0, dk, 0.0).astype(BF16)
        out_ref[2, :, cs] = jnp.where(keep_ref[2, :, cs] > 0, dv_acc[...], 0.0).astype(BF16)


def nn_kernel(ids, *refs):
    *a_refs, w_ref, out_ref = refs
    depth = w_ref.shape[0] // len(a_refs)
    total = dot_nn(a_refs[0][...], w_ref[0:depth])
    for i, a_ref in enumerate(a_refs[1:], 1):
        total += dot_nn(a_ref[...], w_ref[i * depth:(i + 1) * depth])
    out_ref[...] = total


def out_kernel(ids, o_ref, got_ref, w_ref, wz_ref, wc_ref, out_ref):
    total = dot_nn(o_ref[...], w_ref[...])
    first = pl.program_id(0) < pl.num_programs(0) // 2

    @pl.when(first)
    def _():
        out_ref[...] = total + dot_nn(got_ref[...], wz_ref[...])

    @pl.when(jnp.logical_not(first))
    def _():
        out_ref[...] = total + dot_nn(got_ref[...], wc_ref[...])


def combine1_kernel(ids, x_ref, part_ref, h_ref, n2_ref):
    h = (x_ref[...].astype(F32) + part_ref[...]).astype(BF16)
    h_ref[...] = h
    normed, _ = norm_stats(h.astype(F32))
    n2_ref[...] = normed.astype(BF16)


def ffn_kernel(ids, theirs_ref, mine_ref, wu_ref, wg_ref, u_ref, g_ref, act_ref, n2_ref):
    half = theirs_ref.shape[0]

    @pl.when(pl.program_id(0) == 0)
    def _():
        n2_ref[0:half] = theirs_ref[...]
        n2_ref[half:] = mine_ref[...]

    u = dot_nn(n2_ref[...], wu_ref[0])
    g = dot_nn(n2_ref[...], wg_ref[0])
    u_ref[...] = u
    g_ref[...] = g
    act_ref[...] = (g * jax.nn.sigmoid(g) * u).astype(BF16)


def dswiglu_kernel(ids, gy_ref, w_ref, u_ref, g_ref, out_ref):
    grad_act = dot_nt(gy_ref[...], w_ref[...])
    u, g = u_ref[...], g_ref[...]
    sig = jax.nn.sigmoid(g)
    out_ref[0] = (grad_act * (g * sig)).astype(BF16)
    out_ref[1] = (grad_act * u * sig * (1.0 + g * (1.0 - sig))).astype(BF16)


def grad_n2_kernel(ids, lo_ref, hi_ref, w_ref, out_ref):
    depth = lo_ref.shape[2]
    total = dot_nt(lo_ref[0], w_ref[0, :, 0:depth])
    total += dot_nt(hi_ref[0], w_ref[0, :, depth:])
    total += dot_nt(lo_ref[1], w_ref[1, :, 0:depth])
    total += dot_nt(hi_ref[1], w_ref[1, :, depth:])
    out_ref[...] = total


def combine2_kernel(ids, gy_ref, h_ref, part_ref, recv_ref, gh_ref, ghb_ref):
    normed, inv_std = norm_stats(h_ref[...].astype(F32))
    gh = gy_ref[...].astype(F32) + norm_backward(part_ref[...] + recv_ref[...], normed, inv_std)
    gh_ref[...] = gh
    ghb_ref[...] = gh.astype(BF16)


def grad_o_kernel(ids, theirs_ref, mine_ref, w_ref, out_ref):
    half, width = theirs_ref.shape
    lo, hi = slice(0, width // 2), slice(width // 2, width)
    for rows, ref in ((slice(0, half), theirs_ref), (slice(half, 2 * half), mine_ref)):
        out_ref[rows] = (dot_nt(ref[:, lo], w_ref[0]) + dot_nt(ref[:, hi], w_ref[1])).astype(BF16)


def grad_n1_kernel(ids, d_ref, w_ref, out_ref):
    depth = d_ref.shape[2]
    total = dot_nt(d_ref[0], w_ref[:, 0:depth])
    total += dot_nt(d_ref[1], w_ref[:, depth:2 * depth])
    total += dot_nt(d_ref[2], w_ref[:, 2 * depth:])
    out_ref[...] = total


def chip_columns(ref, chip, r):
    return ref[:, pl.ds(pl.multiple_of((chip ^ r) * SHARD, SHARD), SHARD)]


def put_pieces(total, axis, a1_ref, a0_ref, b1_ref, b0_ref):
    piece = [lax.slice_in_dim(total, r * SHARD, (r + 1) * SHARD, axis=axis) for r in range(4)]
    first = pl.program_id(0) < pl.num_programs(0) // 2

    @pl.when(first)
    def _():
        a1_ref[0], a1_ref[1], a0_ref[0], a0_ref[1] = piece[1], piece[3], piece[0], piece[2]

    @pl.when(jnp.logical_not(first))
    def _():
        b1_ref[0], b1_ref[1], b0_ref[0], b0_ref[1] = piece[2], piece[3], piece[0], piece[1]


def wgrad_rows_kernel(ids, t_ref, m_ref, t2_ref, m2_ref, b_ref, b2_ref, a1_ref, a0_ref, b1_ref, b0_ref, at_ref):
    n = t_ref.shape[0]

    @pl.when(pl.program_id(0) == 0)
    def _():
        for r in range(4):
            for i, ref in enumerate((t_ref, m_ref, t2_ref, m2_ref)):
                at_ref[r * SHARD:(r + 1) * SHARD, i * n:(i + 1) * n] = chip_columns(ref, ids[2], r).T

    total = dot_nn(at_ref[:, 0:2 * n], b_ref[0]) + dot_nn(at_ref[:, 2 * n:], b2_ref[0])
    put_pieces(total, 0, a1_ref, a0_ref, b1_ref, b0_ref)


def wgrad_cols_kernel(ids, a_ref, a2_ref, t_ref, m_ref, t2_ref, m2_ref, a1_ref, a0_ref, b1_ref, b0_ref, br_ref):
    n = t_ref.shape[0]

    @pl.when(pl.program_id(0) == 0)
    def _():
        for r in range(4):
            for i, ref in enumerate((t_ref, m_ref, t2_ref, m2_ref)):
                br_ref[i * n:(i + 1) * n, r * SHARD:(r + 1) * SHARD] = chip_columns(ref, ids[2], r)

    total = dot_tn(a_ref[...], br_ref[0:2 * n]) + dot_tn(a2_ref[...], br_ref[2 * n:])
    put_pieces(total, 1, a1_ref, a0_ref, b1_ref, b0_ref)


def add_kernel(ids, a_ref, ra_ref, b_ref, rb_ref, ak_ref, as_ref, bk_ref, bs_ref):
    for own, got, keep, send in ((a_ref, ra_ref, ak_ref, as_ref), (b_ref, rb_ref, bk_ref, bs_ref)):
        keep[...] = own[0] + got[0]
        send[...] = own[1] + got[1]


def final_kernel(ids, *refs):
    *in_refs, out_ref = refs
    for i in range(out_ref.shape[0]):
        out_ref[i] = in_refs[2 * i][...] + in_refs[2 * i + 1][...]


def final_cols_kernel(ids, *refs):
    *in_refs, out_ref = refs
    n = in_refs[0].shape[1]
    for i in range(len(in_refs) // 2):
        out_ref[:, i * n:(i + 1) * n] = in_refs[2 * i][...] + in_refs[2 * i + 1][...]


def final_ff_kernel(ids, *refs):
    *in_refs, out_ref = refs
    n = in_refs[0].shape[1]
    for i in range(len(in_refs) // 2):
        unit, c = i // 2, i % 2
        out_ref[:, c, unit * n:(unit + 1) * n] = in_refs[2 * i][...] + in_refs[2 * i + 1][...]


def natural_order(values):
    n = values.shape[1] // SHARD
    blocks = [values[:, s * SHARD:(s + 1) * SHARD] for s in range(n)]
    return jnp.concatenate([blocks[(b % 2) * (n // 2) + b // 2] for b in range(n)], axis=1)


def y_kernel(ids, h_ref, part_ref, recv_ref, y_ref):
    y = (h_ref[...].astype(F32) + (part_ref[...] + recv_ref[...])).astype(BF16)
    y_ref[...] = natural_order(y)


def gx_kernel(ids, gh_ref, x_ref, part_ref, recv_ref, gx_ref):
    normed, inv_std = norm_stats(x_ref[...].astype(F32))
    gx = gh_ref[...] + norm_backward(part_ref[...] + recv_ref[...], normed, inv_std)
    gx_ref[...] = natural_order(gx.astype(BF16))


def swap(value, axis):
    return lax.ppermute(value, axis, SWAP)


def gather(weight, axis):
    return lax.all_gather(weight, ('c', 'y', 'x'), axis=axis, tiled=True)


def layer(x, grad_y, w_qkv, w_out, w_ff, w_down):
    batch, seq, width = x.shape
    heads, head = w_qkv.shape[2:]
    inner = heads * head
    units = w_ff.shape[2]
    tokens = batch * seq
    half = tokens // 2
    z = lax.axis_index('z')
    ids = jnp.stack([z, lax.axis_index('c'), 2 * lax.axis_index('y') + lax.axis_index('x')]).astype(jnp.int32)
    scale = head ** -0.5

    inv_freq = 10000.0 ** (-jnp.arange(0, head, 2, dtype=F32) / head)
    angles = jnp.arange(seq, dtype=F32)[:, None] * inv_freq[None, :]
    cos_tab = jnp.concatenate([jnp.cos(angles), jnp.cos(angles)], axis=1)
    sin_tab = jnp.concatenate([-jnp.sin(angles), jnp.sin(angles)], axis=1)

    br = 128
    per_half = half // br
    steps = tokens // br
    rows = w_ff.shape[0] // steps
    src = lambda i: (((i // per_half + lax.axis_index('z') + 1) % 2) * per_half + i % per_half, 0)
    row = lambda i, s: (i, 0)
    anywhere = pl.BlockSpec(memory_space=pl.ANY)
    wq = w_qkv.reshape(w_qkv.shape[0], 3 * inner)
    wo = w_out.reshape(inner, w_out.shape[2])
    n1, xp, gyp, ff_t, qkv_full, out_full = call(
        head_kernel, (steps,),
        [pl.BlockSpec((br, width), src)] * 2 + [pl.BlockSpec((rows, 2, units), lambda i: (i, 0, 0))] + [anywhere] * 2,
        [pl.BlockSpec((br, width), lambda i: (i, 0))] * 3 + [pl.BlockSpec((2, rows, units), lambda i: (0, i, 0))] + [anywhere] * 2,
        [sds((tokens, width), BF16)] * 3
        + [sds((2, w_ff.shape[0], units), BF16), sds((width, 3 * inner), BF16), sds((2, inner, width // 2), BF16)],
        None, [x.reshape(tokens, width), grad_y.reshape(tokens, width), w_ff, wq, wo], 20 * tokens * width,
        scratch=[pltpu.VMEM(wq.shape, BF16), pltpu.VMEM(wo.shape, BF16), pltpu.SemaphoreType.DMA((4,)),
                 pltpu.SemaphoreType.DMA((2, ROLES)), pltpu.SemaphoreType.DMA((2, ROLES))], collective=0)
    out_z = swap(lax.dynamic_index_in_dim(out_full, lax.axis_index('c'), 0, keepdims=False), 'z')
    out_zc = swap(out_z, 'c')
    ff_full = gather(ff_t, 1)
    down_full = gather(w_down, 1)

    bn = 512
    fixed = lambda *_: (0, 0)
    n_qkv = 3 * inner // bn
    per = n_qkv // 3
    bh = 256
    n_h = inner // bh

    qkv, keep = call(
        functools.partial(qkv_kernel, rotated=2 * per), (n_qkv,),
        [pl.BlockSpec((tokens, width), fixed), pl.BlockSpec((width, bn), lambda j, s: (0, j)),
         pl.BlockSpec((seq, head), fixed), pl.BlockSpec((seq, head), fixed)],
        [pl.BlockSpec((tokens, bn), lambda j, s: (0, j)), pl.BlockSpec((None, tokens, bn), lambda j, s: (j // per, 0, j % per))],
        [sds((tokens, 3 * inner), BF16), sds((3, tokens, inner), BF16)], ids,
        [n1, qkv_full, cos_tab, sin_tab], 2 * tokens * width * 3 * inner)

    def attn_rows(r, old):
        send = not old
        return call(
            functools.partial(attn_kernel, head=head, scale=scale, rows=256, send=send), (n_h,),
            [pl.BlockSpec((half, bh), lambda h, s, p=p: (r, p * n_h + h)) for p in range(3)] + [anywhere] * len(old),
            [pl.BlockSpec((half, bh), lambda h, s: (0, h))] * send + [pl.BlockSpec((half, bh), lambda h, s: (r, h))],
            [sds((half, inner), BF16)] * send + [sds((tokens, inner), BF16)], ids,
            [qkv, qkv, qkv, *old], 4 * half * seq * inner, aliases={4: 0} if old else None)

    def nn(lhs, w, r):
        depth = lhs[0].shape[1]
        return call(
            nn_kernel, (width // bn,),
            [pl.BlockSpec((half, depth), lambda j, s: (r, 0))] * len(lhs) + [pl.BlockSpec((depth * len(lhs), bn), lambda j, s: (0, j))],
            pl.BlockSpec((half, bn), lambda j, s: (0, j)), sds((half, width), F32), ids,
            [*lhs, w], 2 * half * depth * len(lhs) * width)

    o_theirs, attn_o = attn_rows(0, ())
    o_got = swap(o_theirs, 'z')
    (attn_o,) = attn_rows(1, (attn_o,))
    wn = bn // 2
    nw = width // 2 // wn
    part = call(
        out_kernel, (2 * nw,),
        [pl.BlockSpec((half, inner), lambda j, s: (1, 0)), pl.BlockSpec((half, inner), fixed),
         pl.BlockSpec((None, inner, wn), lambda j, s: ((s[1] + j // nw) % 2, 0, j % nw)),
         pl.BlockSpec((inner, wn), lambda j, s: (0, jnp.minimum(j, nw - 1))), pl.BlockSpec((inner, wn), lambda j, s: (0, jnp.maximum(j - nw, 0)))],
        pl.BlockSpec((half, wn), lambda j, s: (0, (s[1] + j // nw) % 2 * nw + j % nw)), sds((half, width), F32), ids,
        [attn_o, o_got, out_full, out_z, out_zc], 4 * half * inner * width)
    mine_rows = lambda i, s: (per_half + i, 0)
    block = pl.BlockSpec((br, width), row)
    hidden, n2_mine = call(
        combine1_kernel, (per_half,), [pl.BlockSpec((br, width), mine_rows), block], [block, block],
        [sds((half, width), BF16)] * 2, ids, [xp, part], 20 * half * width)
    n2_theirs = swap(n2_mine, 'z')

    bf = 256
    hu = units // 2

    def ffn(k):
        nb = hu // bf
        return call(
            ffn_kernel, (nb,),
            [pl.BlockSpec((half, width), fixed)] * 2
            + [pl.BlockSpec((1, width, bf), lambda j, s, c=c: (c, 0, k * nb + j)) for c in range(2)],
            [pl.BlockSpec((tokens, bf), lambda j, s: (0, j))] * 3,
            [sds((tokens, hu), F32)] * 2 + [sds((tokens, hu), BF16)], ids,
            [n2_theirs, n2_mine, ff_full, ff_full], 4 * tokens * width * hu, scratch=[pltpu.VMEM((tokens, width), BF16)])

    up0, gate0, act0 = ffn(0)
    up1, gate1, act1 = ffn(1)
    act0_sib = swap(act0, 'c')
    act1_sib = swap(act1, 'c')
    gyp_sib = swap(gyp, 'c')
    n1_sib = swap(n1, 'c')
    o_sib = swap(attn_o, 'c')
    n2_mine_sib = swap(n2_mine, 'c')
    n2_theirs_sib = swap(n2_theirs, 'c')

    ba = 512

    def two_halves(value):
        return [(value, r) for r in range(2)]

    def source_specs(sources):
        return [pl.BlockSpec((half, width // 2), lambda i, s, r=r: (r, s[1])) for _, r in sources]

    def wgrad_cols(a, a2, sources):
        n = a.shape[1] // ba
        piece = sds((2, a.shape[1] // 2, SHARD), F32)
        lo = pl.BlockSpec((2, ba, SHARD), lambda i, s: (0, jnp.minimum(i, n // 2 - 1), 0))
        hi = pl.BlockSpec((2, ba, SHARD), lambda i, s: (0, jnp.maximum(i - n // 2, 0), 0))
        return call(
            wgrad_cols_kernel, (n,),
            [pl.BlockSpec((tokens, ba), lambda i, s: (0, i))] * 2 + source_specs(sources), [lo, lo, hi, hi], [piece] * 4, ids,
            [a, a2, *(v for v, _ in sources)], 4 * tokens * a.shape[1] * width // 2,
            scratch=[pltpu.VMEM((2 * tokens, width // 2), BF16)])

    def wgrad_rows(sources, b, b2):
        per_b = b.shape[2] // bn
        n = b.shape[0] * per_b
        piece = sds((2, SHARD, n * bn // 2), F32)
        lo = pl.BlockSpec((2, SHARD, bn), lambda i, s: (0, 0, jnp.minimum(i, n // 2 - 1)))
        hi = pl.BlockSpec((2, SHARD, bn), lambda i, s: (0, 0, jnp.maximum(i - n // 2, 0)))
        return call(
            wgrad_rows_kernel, (n,),
            source_specs(sources) + [pl.BlockSpec((1, tokens, bn), lambda i, s: (i // per_b, 0, i % per_b))] * 2,
            [lo, lo, hi, hi], [piece] * 4, ids, [*(v for v, _ in sources), b, b2], 4 * tokens * width // 2 * n * bn,
            scratch=[pltpu.VMEM((width // 2, 2 * tokens), BF16)])

    def sum_plane(pieces):
        a1, a0, b1, b0 = pieces
        got_a = swap(a1, 'x')
        got_b = swap(b1, 'y')
        r, c = a0.shape[1:]
        blk = min(r, 128 if c > 256 else 1024)
        two = pl.BlockSpec((2, blk, c), lambda i, s: (0, i, 0))
        one = pl.BlockSpec((blk, c), row)
        a_keep, a_send, b_keep, b_send = call(
            add_kernel, (r // blk,), [two] * 4, [one] * 4, [sds((r, c), F32)] * 4, ids,
            [a0, got_a, b0, got_b], 8 * r * c)
        return [a_keep, swap(a_send, 'y'), b_keep, swap(b_send, 'x')]

    def final(pairs):
        r, c = pairs[0].shape
        blk = min(r, 128 if c > 256 else 1024)
        return call(
            final_kernel, (r // blk,), [pl.BlockSpec((blk, c), row)] * len(pairs),
            pl.BlockSpec((len(pairs) // 2, blk, c), lambda i, s: (0, i, 0)), sds((len(pairs) // 2, r, c), F32), ids, pairs, 4 * r * c)

    gy_sources = two_halves(gyp) + two_halves(gyp_sib)
    down0 = sum_plane(wgrad_cols(act0, act0_sib, gy_sources))
    down1 = sum_plane(wgrad_cols(act1, act1_sib, gy_sources))
    grad_down = final(down0 + down1).reshape(units, SHARD)

    def dswiglu(k, up, gate):
        nb = hu // bf
        return call(
            dswiglu_kernel, (nb,),
            [pl.BlockSpec((tokens, width), fixed), pl.BlockSpec((bf, width), lambda j, s: (k * nb + j, 0))]
            + [pl.BlockSpec((tokens, bf), lambda j, s: (0, j))] * 2,
            pl.BlockSpec((2, tokens, bf), lambda j, s: (0, 0, j)), sds((2, tokens, hu), BF16), ids,
            [gyp, down_full, up, gate], 2 * tokens * width * hu)

    d0 = dswiglu(0, up0, gate0)
    d1 = dswiglu(1, up1, gate1)
    d0_sib = swap(d0, 'c')
    d1_sib = swap(d1, 'c')

    def grad_n2(r):
        bd = 256
        return call(
            grad_n2_kernel, (width // bd,),
            [pl.BlockSpec((2, half, hu), lambda j, s: (0, r, 0))] * 2 + [pl.BlockSpec((2, bd, units), lambda j, s: (0, j, 0))],
            pl.BlockSpec((half, bd), lambda j, s: (0, j)), sds((half, width), F32), ids,
            [d0, d1, ff_full], 4 * half * width * units)

    gn2_theirs = grad_n2(0)
    gn2_got = swap(gn2_theirs, 'z')
    n2_sources = [(n2_theirs, 0), (n2_mine, 0), (n2_theirs_sib, 0), (n2_mine_sib, 0)]
    ff0 = sum_plane(wgrad_rows(n2_sources, d0, d0_sib))
    ff1 = sum_plane(wgrad_rows(n2_sources, d1, d1_sib))
    br_ff = 32
    grad_ff = call(
        final_ff_kernel, (SHARD // br_ff,), [pl.BlockSpec((br_ff, hu), row)] * 8,
        pl.BlockSpec((br_ff, 2, units), lambda i, s: (i, 0, 0)), sds((SHARD, 2, units), F32), ids, ff0 + ff1, 4 * SHARD * units)
    gn2_mine = grad_n2(1)

    gh, gh_mine = call(
        combine2_kernel, (per_half,),
        [pl.BlockSpec((br, width), mine_rows), block, block, block], [block, block],
        [sds((half, width), F32), sds((half, width), BF16)], ids,
        [gyp, hidden, gn2_mine, gn2_got], 20 * half * width)
    gh_theirs = swap(gh_mine, 'z')
    y_theirs = nn([act0, act1], down_full, 0)
    y_got = swap(y_theirs, 'z')
    y_mine = nn([act0, act1], down_full, 1)

    grad_o = call(
        grad_o_kernel, (inner // bn,),
        [pl.BlockSpec((half, width), fixed)] * 2 + [pl.BlockSpec((2, bn, width // 2), lambda j, s: (0, j, 0))],
        pl.BlockSpec((tokens, bn), lambda j, s: (0, j)), sds((tokens, inner), BF16), ids,
        [gh_theirs, gh_mine, out_full], 2 * tokens * width * inner)
    gh_theirs_sib = swap(gh_theirs, 'c')
    gh_mine_sib = swap(gh_mine, 'c')
    dqkv = call(
        functools.partial(attn_bwd_kernel, head=head, scale=scale, rows=256), (batch, n_h),
        [pl.BlockSpec((seq, bh), lambda b, h, s, p=p: (b, p * n_h + h)) for p in range(3)]
        + [pl.BlockSpec((seq, bh), lambda b, h, s: (b, h)), pl.BlockSpec((3, seq, bh), lambda b, h, s: (0, b, h)),
           pl.BlockSpec((seq, head), fixed), pl.BlockSpec((seq, head), fixed)],
        pl.BlockSpec((3, seq, bh), lambda b, h, s: (0, b, h)), sds((3, tokens, inner), BF16), ids,
        [qkv, qkv, qkv, grad_o, keep, cos_tab, sin_tab], 10 * tokens * seq * inner,
        scratch=[pltpu.VMEM((seq, head), F32)] * 2)
    dqkv_sib = swap(dqkv, 'c')

    def grad_n1(r):
        return call(
            grad_n1_kernel, (width // bn,),
            [pl.BlockSpec((3, half, inner), lambda j, s: (0, r, 0)), pl.BlockSpec((bn, 3 * inner), lambda j, s: (j, 0))],
            pl.BlockSpec((half, bn), lambda j, s: (0, j)), sds((half, width), F32), ids,
            [dqkv, qkv_full], 2 * half * width * 3 * inner)

    gn1_theirs = grad_n1(0)
    gn1_got = swap(gn1_theirs, 'z')
    gh_sources = [(gh_theirs, 0), (gh_mine, 0), (gh_theirs_sib, 0), (gh_mine_sib, 0)]
    out_pairs = sum_plane(wgrad_cols(attn_o, o_sib, gh_sources))
    grad_out = final(out_pairs).reshape(heads, head, SHARD)
    qkv_pairs = sum_plane(wgrad_rows(two_halves(n1) + two_halves(n1_sib), dqkv, dqkv_sib))
    half_cols = 3 * inner // 2
    grad_qkv = call(
        final_cols_kernel, (2,), [pl.BlockSpec((br, half_cols), row)] * 4,
        pl.BlockSpec((br, 3 * inner), row), sds((SHARD, 3 * inner), F32), ids, qkv_pairs, 4 * SHARD * half_cols)
    grad_qkv = grad_qkv.reshape(SHARD, 3, heads, head)
    gn1_mine = grad_n1(1)

    def in_order(theirs, mine):
        both = jnp.where(z == 0, jnp.concatenate([mine, theirs], 0), jnp.concatenate([theirs, mine], 0))
        return both.reshape(batch, seq, width)

    y_own = call(
        y_kernel, (per_half,), [block] * 3, block, sds((half, width), BF16), ids, [hidden, y_mine, y_got], 4 * half * width)
    y_out = in_order(swap(y_own, 'z'), y_own)
    gx_own = call(
        gx_kernel, (per_half,), [block, pl.BlockSpec((br, width), mine_rows), block, block], block,
        sds((half, width), BF16), ids, [gh, xp, gn1_mine, gn1_got], 20 * half * width)
    grad_x = in_order(swap(gx_own, 'z'), gx_own)
    return y_out, grad_x, grad_qkv, grad_out, grad_ff, grad_down


def solution(mesh):
    fine = Mesh(np.asarray(mesh.devices).reshape(2, 2, 2, 2), ('z', 'y', 'x', 'c'))
    fsdp = ('y', 'x', 'c')
    act_spec = P(fsdp, None, None)
    weight_specs = (P(fsdp, None, 'z', None), P('z', None, fsdp), P(fsdp, None, 'z'), P('z', fsdp))
    return jax.shard_map(layer, mesh=fine, in_specs=(act_spec, act_spec) + weight_specs, out_specs=(act_spec, act_spec) + weight_specs, check_vma=False)
```
